8 devices in a mesh: dp: 1 (over z), wg: 8 (over y, x, core).
Axes of the slice: x: 2, y: 2, z: 1, core: 2. Of those that a mesh axis runs over, the one named last changes fastest.
Arguments:
- hidden: bfloat16 [32, 384, 6144], P(('dp', 'wg'))
- seq_lens: int32 [32], P(('dp', 'wg'))
- route_idx: int32 [12288, 2], P(('dp', 'wg'))
- g_attn_in: bfloat16 [6144], P('wg')
- w_query: bfloat16 [6144, 6144], P('wg')
- w_key: bfloat16 [6144, 1024], P('wg')
- w_value: bfloat16 [6144, 1024], P('wg')
- w_attn_out: bfloat16 [6144, 6144], P('wg')
- g_attn_out: bfloat16 [6144], P('wg')
- g_moe_in: bfloat16 [6144], P('wg')
- w_router: bfloat16 [6144, 8], P('wg')
- w_gate: bfloat16 [8, 6144, 1024], P(None, 'wg')
- w_up: bfloat16 [8, 6144, 1024], P(None, 'wg')
- w_down: bfloat16 [8, 1024, 6144], P(None, 'wg')
- g_moe_out: bfloat16 [6144], P('wg')
Outputs:
- output 1: bfloat16 [32, 384, 6144], P(('dp', 'wg'))
- output 2: bfloat16 [32, 384, 8, 128], P(('dp', 'wg'))
- output 3: bfloat16 [32, 384, 8, 128], P(('dp', 'wg'))
All inputs are finite; a program needn't handle non-finite values.
Results may differ from the reference program's by a relative error of at most 0.02.
Values are sent between devices in bfloat16 or wider.
A program may use at most 1 GiB of HBM per device.

```python
import jax
import jax.numpy as jnp
from jax import lax

D_MODEL = 6144
HEADS = 48
KV_HEADS = 8
HEAD_DIM = 128
EXPERTS = 8
TOP_K = 2
FF_DIM = 1024
SEQ_LEN = 384
BATCH = 32
TOKENS_DEV = 1536

SOFT_CAP = 30.0
NORM_EPS = 1e-5
ROPE_BASE = 10000.0
ATTN_SCALE = HEAD_DIM ** -0.5
GROUPS = HEADS // KV_HEADS
N_ROWS = BATCH * SEQ_LEN


def normal_weight(key_w, out_shape, w_scale):
    return (jax.random.normal(key_w, out_shape, jnp.float32) * w_scale).astype(jnp.bfloat16)


def setup_inputs(seed: int = 0, part: int = 0) -> dict:
    root_key = jax.random.key(seed)
    part_key = jax.random.fold_in(jax.random.key(seed + 1), part)
    w_keys = jax.random.split(root_key, 9)
    p_keys = jax.random.split(part_key, 7)
    in_scale = D_MODEL ** -0.5
    hidden = jax.random.normal(p_keys[0], (BATCH, SEQ_LEN, D_MODEL), jnp.float32).astype(jnp.bfloat16)
    seq_lens = jax.random.randint(p_keys[1], (BATCH,), SEQ_LEN // 4, SEQ_LEN + 1)
    len_picks = jax.random.permutation(p_keys[2], BATCH)
    seq_lens = seq_lens.at[len_picks[0]].set(SEQ_LEN).at[len_picks[1]].set(SEQ_LEN // 4).astype(jnp.int32)
    draw_a = jax.random.randint(p_keys[3], (N_ROWS,), 0, EXPERTS)
    draw_b = jax.random.randint(p_keys[4], (N_ROWS,), 0, EXPERTS)
    shift_amt = jax.random.randint(p_keys[5], (), 0, EXPERTS)
    local_pos = jnp.arange(N_ROWS) % TOKENS_DEV
    first_pick = jnp.where(local_pos < EXPERTS, (local_pos + shift_amt) % EXPERTS, jnp.minimum(draw_a, draw_b))
    second_pick = (first_pick + jax.random.randint(p_keys[6], (N_ROWS,), 1, EXPERTS)) % EXPERTS
    route_idx = jnp.stack([first_pick, second_pick], axis=1).astype(jnp.int32)
    gain_rows = (1.0 + 0.3 * jax.random.normal(w_keys[7], (4, D_MODEL), jnp.float32)).astype(jnp.bfloat16)
    return {
        'hidden': hidden,
        'seq_lens': seq_lens,
        'route_idx': route_idx,
        'g_attn_in': gain_rows[0],
        'w_query': normal_weight(w_keys[0], (D_MODEL, HEADS * HEAD_DIM), 3.0 * in_scale),
        'w_key': normal_weight(w_keys[1], (D_MODEL, KV_HEADS * HEAD_DIM), 3.0 * in_scale),
        'w_value': normal_weight(w_keys[2], (D_MODEL, KV_HEADS * HEAD_DIM), in_scale),
        'w_attn_out': normal_weight(w_keys[3], (HEADS * HEAD_DIM, D_MODEL), (HEADS * HEAD_DIM) ** -0.5),
        'g_attn_out': gain_rows[1],
        'g_moe_in': gain_rows[2],
        'w_router': normal_weight(w_keys[4], (D_MODEL, EXPERTS), in_scale),
        'w_gate': normal_weight(w_keys[5], (EXPERTS, D_MODEL, FF_DIM), in_scale),
        'w_up': normal_weight(w_keys[6], (EXPERTS, D_MODEL, FF_DIM), in_scale),
        'w_down': normal_weight(w_keys[8], (EXPERTS, FF_DIM, D_MODEL), FF_DIM ** -0.5),
        'g_moe_out': gain_rows[3],
    }


def rms_norm(values, gain_vec):
    values_f32 = values.astype(jnp.float32)
    inv_rms = lax.rsqrt(jnp.mean(values_f32 * values_f32, axis=-1, keepdims=True) + NORM_EPS)
    return values_f32 * inv_rms * gain_vec.astype(jnp.float32)


def apply_rope(values, cos_t, sin_t):
    half_dim = HEAD_DIM // 2
    values_f32 = values.astype(jnp.float32)
    first_half = values_f32[..., :half_dim]
    second_half = values_f32[..., half_dim:]
    return jnp.concatenate([first_half * cos_t - second_half * sin_t, second_half * cos_t + first_half * sin_t], axis=-1).astype(jnp.bfloat16)


def reference(hidden, seq_lens, route_idx, g_attn_in, w_query, w_key, w_value, w_attn_out, g_attn_out, g_moe_in, w_router, w_gate, w_up, w_down, g_moe_out):
    half_dim = HEAD_DIM // 2
    inv_freq = ROPE_BASE ** (-jnp.arange(half_dim, dtype=jnp.float32) * (2.0 / HEAD_DIM))
    angles = jnp.arange(SEQ_LEN, dtype=jnp.float32)[:, None] * inv_freq[None, :]
    cos_t = jnp.cos(angles)[:, None, :]
    sin_t = jnp.sin(angles)[:, None, :]
    positions = jnp.arange(SEQ_LEN)
    expert_ids = jnp.arange(EXPERTS)

    def layer_prompt(operands):
        tok_rows, length, choice = operands
        h_attn = rms_norm(tok_rows, g_attn_in).astype(jnp.bfloat16)
        q_proj = jnp.dot(h_attn, w_query, preferred_element_type=jnp.float32).astype(jnp.bfloat16)
        k_proj = jnp.dot(h_attn, w_key, preferred_element_type=jnp.float32).astype(jnp.bfloat16)
        v_proj = jnp.dot(h_attn, w_value, preferred_element_type=jnp.float32).astype(jnp.bfloat16)
        q_rope = apply_rope(q_proj.reshape(SEQ_LEN, HEADS, HEAD_DIM), cos_t, sin_t).reshape(SEQ_LEN, KV_HEADS, GROUPS, HEAD_DIM)
        k_rope = apply_rope(k_proj.reshape(SEQ_LEN, KV_HEADS, HEAD_DIM), cos_t, sin_t)
        v_heads = v_proj.reshape(SEQ_LEN, KV_HEADS, HEAD_DIM)
        scores = jnp.einsum('qkgd,skd->kgqs', q_rope.astype(jnp.float32), k_rope.astype(jnp.float32)) * ATTN_SCALE
        scores = SOFT_CAP * jnp.tanh(scores / SOFT_CAP)
        allowed = (positions[None, :] <= positions[:, None]) & (positions[None, :] < length)
        scores = jnp.where(allowed, scores, -1e30)
        attn_probs = jax.nn.softmax(scores, axis=-1).astype(jnp.bfloat16)
        context = jnp.einsum('kgqs,skd->qkgd', attn_probs.astype(jnp.float32), v_heads.astype(jnp.float32)).astype(jnp.bfloat16)
        attn_out = jnp.dot(context.reshape(SEQ_LEN, HEADS * HEAD_DIM), w_attn_out, preferred_element_type=jnp.float32)
        mid_rows = (tok_rows.astype(jnp.float32) + rms_norm(attn_out, g_attn_out)).astype(jnp.bfloat16)
        h_moe = rms_norm(mid_rows, g_moe_in).astype(jnp.bfloat16)
        router_probs = jax.nn.softmax(jnp.dot(h_moe, w_router, preferred_element_type=jnp.float32), axis=-1)
        gate_probs = jnp.take_along_axis(router_probs, choice, axis=1)
        combine = jnp.sum(gate_probs[:, :, None] * (choice[:, :, None] == expert_ids).astype(jnp.float32), axis=1)

        def expert_step(moe_acc, expert_ops):
            w_gate_e, w_up_e, w_down_e, weight_col = expert_ops
            gate_act = jnp.dot(h_moe, w_gate_e, preferred_element_type=jnp.float32)
            up_act = jnp.dot(h_moe, w_up_e, preferred_element_type=jnp.float32)
            inner_act = (jax.nn.gelu(gate_act) * up_act).astype(jnp.bfloat16)
            expert_out = jnp.dot(inner_act, w_down_e, preferred_element_type=jnp.float32)
            return moe_acc + weight_col[:, None] * expert_out, None

        moe_out = lax.scan(expert_step, jnp.zeros((SEQ_LEN, D_MODEL), jnp.float32), (w_gate, w_up, w_down, combine.T))[0]
        y_rows = (mid_rows.astype(jnp.float32) + rms_norm(moe_out, g_moe_out)).astype(jnp.bfloat16)
        return y_rows, k_rope, v_heads

    y_out, k_cache, v_cache = lax.map(layer_prompt, (hidden, seq_lens, route_idx.reshape(BATCH, SEQ_LEN, TOP_K)))
    return y_out, k_cache, v_cache
```

```python
import functools
import jax
import jax.numpy as jnp
from jax import lax
from jax.sharding import PartitionSpec as P

HEAD_DIM = 128
SOFT_CAP = 30.0
NORM_EPS = 1e-5
ROPE_BASE = 10000.0
ATTN_SCALE = HEAD_DIM ** -0.5


def dot_f32(left_op, right_op):
    return jnp.dot(left_op, right_op, preferred_element_type=jnp.float32)


def rms_norm(values, gain_vec):
    values_f32 = values.astype(jnp.float32)
    inv_rms = lax.rsqrt(jnp.mean(values_f32 * values_f32, axis=-1, keepdims=True) + NORM_EPS)
    return values_f32 * inv_rms * gain_vec.astype(jnp.float32)


def rope_tables(seq_len):
    half_dim = HEAD_DIM // 2
    inv_freq = ROPE_BASE ** (-jnp.arange(half_dim, dtype=jnp.float32) * (2.0 / HEAD_DIM))
    angles = jnp.arange(seq_len, dtype=jnp.float32)[:, None] * inv_freq[None, :]
    return jnp.cos(angles)[:, None, :], jnp.sin(angles)[:, None, :]


def apply_rope(values, cos_t, sin_t):
    half_dim = HEAD_DIM // 2
    values_f32 = values.astype(jnp.float32)
    first_half = values_f32[..., :half_dim]
    second_half = values_f32[..., half_dim:]
    return jnp.concatenate([first_half * cos_t - second_half * sin_t, second_half * cos_t + first_half * sin_t], axis=-1).astype(jnp.bfloat16)


def attend_prompt(operands):
    q_rows, k_rows, v_rows, length = operands
    positions = jnp.arange(q_rows.shape[0])
    scores = jnp.einsum('qkgd,skd->kgqs', q_rows, k_rows, preferred_element_type=jnp.float32) * ATTN_SCALE
    scores = SOFT_CAP * jnp.tanh(scores / SOFT_CAP)
    allowed = (positions[None, :] <= positions[:, None]) & (positions[None, :] < length)
    scores = jnp.where(allowed, scores, -1e30)
    attn_probs = jax.nn.softmax(scores, axis=-1).astype(jnp.bfloat16)
    return jnp.einsum('kgqs,skd->qkgd', attn_probs, v_rows, preferred_element_type=jnp.float32).astype(jnp.bfloat16)


def attend_rows(q_proj, k_proj, v_proj, seq_lens):
    n_prompts = seq_lens.shape[0]
    seq_len = q_proj.shape[0] // n_prompts
    n_heads = q_proj.shape[1] // HEAD_DIM
    n_kv = k_proj.shape[1] // HEAD_DIM
    cos_t, sin_t = rope_tables(seq_len)
    q_rope = apply_rope(q_proj.reshape(n_prompts, seq_len, n_heads, HEAD_DIM), cos_t, sin_t)
    k_rope = apply_rope(k_proj.reshape(n_prompts, seq_len, n_kv, HEAD_DIM), cos_t, sin_t)
    v_heads = v_proj.reshape(n_prompts, seq_len, n_kv, HEAD_DIM)
    q_groups = q_rope.reshape(n_prompts, seq_len, n_kv, n_heads // n_kv, HEAD_DIM)
    context = lax.map(attend_prompt, (q_groups, k_rope, v_heads, seq_lens))
    return context.reshape(n_prompts * seq_len, n_heads * HEAD_DIM), k_rope, v_heads


def solution(mesh):
    row_spec = P(('dp', 'wg'))
    dim0_spec = P('wg', None)
    dim1_spec = P(None, 'wg', None)
    gather_dim0 = functools.partial(lax.all_gather, axis_name='wg', axis=0, tiled=True)
    gather_dim1 = functools.partial(lax.all_gather, axis_name='wg', axis=1, tiled=True)

    def device_fn(hidden, seq_lens, route_idx, g_attn_in, w_query, w_key, w_value, w_attn_out, g_attn_out, g_moe_in, w_router, w_gate, w_up, w_down, g_moe_out):
        n_prompts, seq_len, d_model = hidden.shape
        n_experts = w_gate.shape[0]
        half = n_experts // 2
        tok_rows = hidden.reshape(n_prompts * seq_len, d_model)
        small = jnp.concatenate([g_attn_in, g_attn_out, g_moe_in, g_moe_out, w_router.T.reshape(-1)])
        small = lax.all_gather(small, 'wg', axis=0, tiled=False)
        n_dev = small.shape[0]
        small = small.reshape(n_dev, 4 + n_experts, -1).transpose(1, 0, 2).reshape(4 + n_experts, d_model)
        h_attn = rms_norm(tok_rows, small[0]).astype(jnp.bfloat16)
        q_proj = dot_f32(h_attn, gather_dim0(w_query)).astype(jnp.bfloat16)
        k_proj = dot_f32(h_attn, gather_dim0(w_key)).astype(jnp.bfloat16)
        v_proj = dot_f32(h_attn, gather_dim0(w_value)).astype(jnp.bfloat16)
        context_rows, k_rope, v_heads = attend_rows(q_proj, k_proj, v_proj, seq_lens)
        attn_out = dot_f32(context_rows, gather_dim0(w_attn_out))
        mid_rows = (tok_rows.astype(jnp.float32) + rms_norm(attn_out, small[1])).astype(jnp.bfloat16)
        h_moe = rms_norm(mid_rows, small[2]).astype(jnp.bfloat16)
        logits = lax.dot_general(h_moe, small[4:], (((1,), (1,)), ((), ())), preferred_element_type=jnp.float32)
        router_probs = jax.nn.softmax(logits, axis=-1)
        picks = (route_idx[:, :, None] == jnp.arange(n_experts)).astype(jnp.float32)
        combine = router_probs * jnp.sum(picks, axis=1)

        def inner(wg, wu):
            gate_act = dot_f32(h_moe, wg)
            up_act = dot_f32(h_moe, wu)
            return (jax.nn.gelu(gate_act) * up_act).astype(jnp.bfloat16)

        moe_out = None
        groups = [(0, half, [(0, half)]), (half, n_experts, [(half, n_experts - 1), (n_experts - 1, n_experts)])]
        for lo, hi, downs in groups:
            wg = gather_dim1(w_gate[lo:hi])
            wu = gather_dim1(w_up[lo:hi])
            wd = [(a, gather_dim1(w_down[a:b])) for a, b in downs]
            acts = [inner(wg[e - lo], wu[e - lo]) for e in range(lo, hi)]
            for a, w_part in wd:
                for j in range(w_part.shape[0]):
                    e = a + j
                    term = combine[:, e:e + 1] * dot_f32(acts[e - lo], w_part[j])
                    moe_out = term if moe_out is None else lax.optimization_barrier(moe_out + term)
        y_rows = (mid_rows.astype(jnp.float32) + rms_norm(moe_out, small[3])).astype(jnp.bfloat16)
        return y_rows.reshape(hidden.shape), k_rope, v_heads

    return jax.shard_map(
        device_fn,
        mesh=mesh,
        in_specs=(row_spec, row_spec, row_spec, P('wg'), dim0_spec, dim0_spec, dim0_spec, dim0_spec, P('wg'), P('wg'), dim0_spec, dim1_spec, dim1_spec, dim1_spec, P('wg')),
        out_specs=(row_spec, row_spec, row_spec),
        check_vma=False,
    )
```

```python
import functools
import jax
import jax.numpy as jnp
from jax import lax
from jax.experimental import pallas as pl
from jax.experimental.pallas import tpu as pltpu
from jax.sharding import PartitionSpec as P

HEAD_DIM = 128
SOFT_CAP = 30.0
NORM_EPS = 1e-5
ROPE_BASE = 10000.0
ATTN_SCALE = HEAD_DIM ** -0.5


def dot_f32(left_op, right_op):
    return jnp.dot(left_op, right_op, preferred_element_type=jnp.float32)


def rms_norm(values, gain_vec):
    values_f32 = values.astype(jnp.float32)
    inv_rms = lax.rsqrt(jnp.mean(values_f32 * values_f32, axis=-1, keepdims=True) + NORM_EPS)
    return values_f32 * inv_rms * gain_vec.astype(jnp.float32)


def rope_tables(seq_len):
    half_dim = HEAD_DIM // 2
    inv_freq = ROPE_BASE ** (-jnp.arange(half_dim, dtype=jnp.float32) * (2.0 / HEAD_DIM))
    angles = jnp.arange(seq_len, dtype=jnp.float32)[:, None] * inv_freq[None, :]
    return jnp.cos(angles)[:, None, :], jnp.sin(angles)[:, None, :]


def apply_rope(values, cos_t, sin_t):
    half_dim = HEAD_DIM // 2
    values_f32 = values.astype(jnp.float32)
    first_half = values_f32[..., :half_dim]
    second_half = values_f32[..., half_dim:]
    return jnp.concatenate([first_half * cos_t - second_half * sin_t, second_half * cos_t + first_half * sin_t], axis=-1).astype(jnp.bfloat16)


def attend_prompt(operands):
    q_rows, k_rows, v_rows, length = operands
    positions = jnp.arange(q_rows.shape[0])
    scores = jnp.einsum('qkgd,skd->kgqs', q_rows, k_rows, preferred_element_type=jnp.float32) * ATTN_SCALE
    scores = SOFT_CAP * jnp.tanh(scores / SOFT_CAP)
    allowed = (positions[None, :] <= positions[:, None]) & (positions[None, :] < length)
    scores = jnp.where(allowed, scores, -1e30)
    attn_probs = jax.nn.softmax(scores, axis=-1).astype(jnp.bfloat16)
    return jnp.einsum('kgqs,skd->qkgd', attn_probs, v_rows, preferred_element_type=jnp.float32).astype(jnp.bfloat16)


def attend_rows(q_proj, k_proj, v_proj, seq_lens):
    n_prompts = seq_lens.shape[0]
    seq_len = q_proj.shape[0] // n_prompts
    n_heads = q_proj.shape[1] // HEAD_DIM
    n_kv = k_proj.shape[1] // HEAD_DIM
    cos_t, sin_t = rope_tables(seq_len)
    q_rope = apply_rope(q_proj.reshape(n_prompts, seq_len, n_heads, HEAD_DIM), cos_t, sin_t)
    k_rope = apply_rope(k_proj.reshape(n_prompts, seq_len, n_kv, HEAD_DIM), cos_t, sin_t)
    v_heads = v_proj.reshape(n_prompts, seq_len, n_kv, HEAD_DIM)
    q_groups = q_rope.reshape(n_prompts, seq_len, n_kv, n_heads // n_kv, HEAD_DIM)
    context = lax.map(attend_prompt, (q_groups, k_rope, v_heads, seq_lens))
    return context.reshape(n_prompts * seq_len, n_heads * HEAD_DIM), k_rope, v_heads


def group_down_kernel(n_act, has_acc, *refs):
    act_refs = refs[:n_act]
    weight_ref, comb_ref = refs[n_act:n_act + 2]
    acc_ref = refs[n_act + 2] if has_acc else None
    out_ref = refs[-1]
    block = 512

    @pl.loop(0, out_ref.shape[0] // block)
    def _(m):
        rows = pl.ds(pl.multiple_of(m * block, block), block)
        total = acc_ref[rows, :] if has_acc else None
        for i in range(n_act):
            term = comb_ref[rows, i:i + 1] * dot_f32(act_refs[i][rows, :], weight_ref[i])
            total = term if total is None else total + term
        out_ref[rows, :] = total


def group_down(acts, weights, comb, acc):
    n_act = len(acts)
    rows, ff = acts[0].shape
    d_model = weights.shape[2]
    block = 512
    col_map = lambda n: (0, n)
    whole_map = lambda n: (0, 0)
    in_specs = [pl.BlockSpec((rows, ff), whole_map, pipeline_mode=pl.Buffered(1)) for _ in acts]
    in_specs.append(pl.BlockSpec((n_act, ff, block), lambda n: (0, 0, n)))
    in_specs.append(pl.BlockSpec((rows, n_act), whole_map))
    operands = [*acts, weights, comb]
    if acc is not None:
        in_specs.append(pl.BlockSpec((rows, block), col_map))
        operands.append(acc)
    return pl.pallas_call(
        functools.partial(group_down_kernel, n_act, acc is not None),
        grid=(d_model // block,),
        in_specs=in_specs,
        out_specs=pl.BlockSpec((rows, block), col_map),
        out_shape=jax.ShapeDtypeStruct((rows, d_model), jnp.float32),
        compiler_params=pltpu.CompilerParams(vmem_limit_bytes=60 * 1024 * 1024),
        cost_estimate=pl.CostEstimate(flops=2 * n_act * rows * ff * d_model, bytes_accessed=rows * d_model * 8, transcendentals=0),
        name='group_down',
    )(*operands)


def last_down_kernel(act_ref, weight_ref, comb_ref, acc_ref, mid_ref, gain_ref, out_ref, sum_ref):
    d_model = out_ref.shape[1]
    step = d_model // 6
    square_sum = jnp.zeros((out_ref.shape[0], 1), jnp.float32)
    for j in range(6):
        cols = slice(j * step, (j + 1) * step)
        part = acc_ref[:, cols] + comb_ref[...] * dot_f32(act_ref[...], weight_ref[:, cols])
        sum_ref[:, cols] = part
        square_sum += jnp.sum(part * part, axis=-1, keepdims=True)
    inv_rms = lax.rsqrt(square_sum * (1.0 / d_model) + NORM_EPS)
    for j in range(6):
        cols = slice(j * step, (j + 1) * step)
        out_ref[:, cols] = (mid_ref[:, cols].astype(jnp.float32) + sum_ref[:, cols] * inv_rms * gain_ref[:, cols]).astype(jnp.bfloat16)


def last_down(act, weight, comb, acc, mid, gain):
    rows, ff = act.shape
    d_model = weight.shape[1]
    block = 256
    row_map = lambda m: (m, 0)
    whole_map = lambda m: (0, 0)
    return pl.pallas_call(
        last_down_kernel,
        grid=(rows // block,),
        in_specs=[
            pl.BlockSpec((block, ff), row_map),
            pl.BlockSpec((ff, d_model), whole_map, pipeline_mode=pl.Buffered(1)),
            pl.BlockSpec((block, 1), row_map),
            pl.BlockSpec((block, d_model), row_map),
            pl.BlockSpec((block, d_model), row_map),
            pl.BlockSpec((1, d_model), whole_map),
        ],
        out_specs=pl.BlockSpec((block, d_model), row_map),
        out_shape=jax.ShapeDtypeStruct((rows, d_model), jnp.bfloat16),
        scratch_shapes=[pltpu.VMEM((block, d_model), jnp.float32)],
        compiler_params=pltpu.CompilerParams(vmem_limit_bytes=60 * 1024 * 1024),
        cost_estimate=pl.CostEstimate(flops=2 * rows * ff * d_model, bytes_accessed=rows * d_model * 8, transcendentals=0),
        name='last_down',
    )(act, weight, comb, acc, mid, gain)


def solution(mesh):
    row_spec = P(('dp', 'wg'))
    dim0_spec = P('wg', None)
    dim1_spec = P(None, 'wg', None)
    gather_dim0 = functools.partial(lax.all_gather, axis_name='wg', axis=0, tiled=True)
    gather_dim1 = functools.partial(lax.all_gather, axis_name='wg', axis=1, tiled=True)

    def device_fn(hidden, seq_lens, route_idx, g_attn_in, w_query, w_key, w_value, w_attn_out, g_attn_out, g_moe_in, w_router, w_gate, w_up, w_down, g_moe_out):
        n_prompts, seq_len, d_model = hidden.shape
        n_experts, local_rows, ff_dim = w_gate.shape
        kv_dim = w_key.shape[1]
        tok_rows = hidden.reshape(n_prompts * seq_len, d_model)
        small = jnp.concatenate([g_attn_in, g_attn_out, g_moe_in, g_moe_out, w_router.T.reshape(-1)])
        small = lax.all_gather(small, 'wg', axis=0, tiled=False)
        n_dev = small.shape[0]
        small = small.reshape(n_dev, 4 + n_experts, -1).transpose(1, 0, 2).reshape(4 + n_experts, d_model)
        h_attn = rms_norm(tok_rows, small[0]).astype(jnp.bfloat16)
        q_proj = dot_f32(h_attn, gather_dim0(w_query)).astype(jnp.bfloat16)
        q_proj, h_attn = lax.optimization_barrier((q_proj, h_attn))
        kv_proj = dot_f32(h_attn, gather_dim0(jnp.concatenate([w_key, w_value], axis=1))).astype(jnp.bfloat16)
        k_proj, v_proj = kv_proj[:, :kv_dim], kv_proj[:, kv_dim:]
        context_rows, k_rope, v_heads = attend_rows(q_proj, k_proj, v_proj, seq_lens)
        attn_out = dot_f32(context_rows, gather_dim0(w_attn_out))
        mid_rows = (tok_rows.astype(jnp.float32) + rms_norm(attn_out, small[1])).astype(jnp.bfloat16)
        h_moe = rms_norm(mid_rows, small[2]).astype(jnp.bfloat16)
        logits = lax.dot_general(h_moe, small[4:], (((1,), (1,)), ((), ())), preferred_element_type=jnp.float32)
        router_probs = jax.nn.softmax(logits, axis=-1)
        picks = (route_idx[:, :, None] == jnp.arange(n_experts)).astype(jnp.float32)
        combine = router_probs * jnp.sum(picks, axis=1)

        def inner(h_in, w_gate_e, w_up_e):
            gate_act = dot_f32(h_in, w_gate_e)
            up_act = dot_f32(h_in, w_up_e)
            return (jax.nn.gelu(gate_act) * up_act).astype(jnp.bfloat16)

        acts = []
        for lo, hi in ((0, 4), (4, 8)):
            n_part = hi - lo
            packed = gather_dim1(jnp.concatenate([w_gate[lo:hi], w_up[lo:hi]], axis=0))
            for i in range(n_part):
                act = inner(h_moe, packed[i], packed[n_part + i])
                act, h_moe = lax.optimization_barrier((act, h_moe))
                acts.append(act)
        *acts, = lax.optimization_barrier(tuple(acts))
        moe_acc = None
        for lo, hi in ((0, 4), (4, 7)):
            moe_acc = group_down(acts[lo:hi], gather_dim1(w_down[lo:hi]), combine[:, lo:hi], moe_acc)
        act_7, down_7 = acts[7], gather_dim1(w_down[7:8])[0]
        y_rows = last_down(act_7, down_7, combine[:, 7:8], moe_acc, mid_rows, small[3].astype(jnp.float32)[None])
        return y_rows.reshape(hidden.shape), k_rope, v_heads

    return jax.shard_map(
        device_fn,
        mesh=mesh,
        in_specs=(row_spec, row_spec, row_spec, P('wg'), dim0_spec, dim0_spec, dim0_spec, dim0_spec, P('wg'), P('wg'), dim0_spec, dim1_spec, dim1_spec, dim1_spec, P('wg')),
        out_specs=(row_spec, row_spec, row_spec),
        check_vma=False,
    )
```

```python
import functools
import jax
import jax.numpy as jnp
from jax import lax
from jax.experimental import pallas as pl
from jax.experimental.pallas import tpu as pltpu
from jax.sharding import PartitionSpec as P

HEAD_DIM = 128
SOFT_CAP = 30.0
NORM_EPS = 1e-5
ROPE_BASE = 10000.0
ATTN_SCALE = HEAD_DIM ** -0.5


def dot_f32(left_op, right_op):
    return jnp.dot(left_op, right_op, preferred_element_type=jnp.float32)


def rms_norm(values, gain_vec):
    values_f32 = values.astype(jnp.float32)
    inv_rms = lax.rsqrt(jnp.mean(values_f32 * values_f32, axis=-1, keepdims=True) + NORM_EPS)
    return values_f32 * inv_rms * gain_vec.astype(jnp.float32)


def rope_tables(seq_len):
    half_dim = HEAD_DIM // 2
    inv_freq = ROPE_BASE ** (-jnp.arange(half_dim, dtype=jnp.float32) * (2.0 / HEAD_DIM))
    angles = jnp.arange(seq_len, dtype=jnp.float32)[:, None] * inv_freq[None, :]
    return jnp.cos(angles)[:, None, :], jnp.sin(angles)[:, None, :]


def apply_rope(values, cos_t, sin_t):
    half_dim = HEAD_DIM // 2
    values_f32 = values.astype(jnp.float32)
    first_half = values_f32[..., :half_dim]
    second_half = values_f32[..., half_dim:]
    return jnp.concatenate([first_half * cos_t - second_half * sin_t, second_half * cos_t + first_half * sin_t], axis=-1).astype(jnp.bfloat16)


def attend_prompt(operands):
    q_rows, k_rows, v_rows, length = operands
    positions = jnp.arange(q_rows.shape[0])
    scores = jnp.einsum('qkgd,skd->kgqs', q_rows, k_rows, preferred_element_type=jnp.float32) * ATTN_SCALE
    scores = SOFT_CAP * jnp.tanh(scores / SOFT_CAP)
    allowed = (positions[None, :] <= positions[:, None]) & (positions[None, :] < length)
    scores = jnp.where(allowed, scores, -1e30)
    attn_probs = jax.nn.softmax(scores, axis=-1).astype(jnp.bfloat16)
    return jnp.einsum('kgqs,skd->qkgd', attn_probs, v_rows, preferred_element_type=jnp.float32).astype(jnp.bfloat16)


def attend_rows(q_proj, k_proj, v_proj, seq_lens):
    n_prompts = seq_lens.shape[0]
    seq_len = q_proj.shape[0] // n_prompts
    n_heads = q_proj.shape[1] // HEAD_DIM
    n_kv = k_proj.shape[1] // HEAD_DIM
    cos_t, sin_t = rope_tables(seq_len)
    q_rope = apply_rope(q_proj.reshape(n_prompts, seq_len, n_heads, HEAD_DIM), cos_t, sin_t)
    k_rope = apply_rope(k_proj.reshape(n_prompts, seq_len, n_kv, HEAD_DIM), cos_t, sin_t)
    v_heads = v_proj.reshape(n_prompts, seq_len, n_kv, HEAD_DIM)
    q_groups = q_rope.reshape(n_prompts, seq_len, n_kv, n_heads // n_kv, HEAD_DIM)
    context = lax.map(attend_prompt, (q_groups, k_rope, v_heads, seq_lens))
    return context.reshape(n_prompts * seq_len, n_heads * HEAD_DIM), k_rope, v_heads


PIECE_ORDER = (0, 2, 4, 6, 1, 3, 5, 7)


def swap(values, distance):
    return lax.ppermute(values, 'wg', [(d, d ^ distance) for d in range(8)])


def spread(piece, over_y):
    from_x, from_y = swap(piece, 2), swap(piece, 4)
    from_diag = swap(from_x, 4) if over_y else swap(from_y, 2)
    own = [piece, from_x, from_y, from_diag]
    return own + [swap(part, 1) for part in own]


def owner_columns(values, chunk, start, width):
    me = lax.axis_index('wg')
    return [lax.dynamic_slice_in_dim(values, (me ^ o) * chunk + start, width, axis=1) for o in PIECE_ORDER]


def group_down_kernel(n_act, n_weight, has_acc, *refs):
    act_refs = refs[:n_act]
    weight_refs = [ref.at[i] for ref in refs[n_act:n_act + n_weight] for i in range(ref.shape[0])]
    comb_ref = refs[n_act + n_weight]
    acc_ref = refs[n_act + n_weight + 1] if has_acc else None
    out_ref = refs[-1]
    block = 512

    @pl.loop(0, out_ref.shape[0] // block)
    def _(m):
        rows = pl.ds(pl.multiple_of(m * block, block), block)
        total = acc_ref[rows, :] if has_acc else None
        for i in range(n_act):
            term = comb_ref[rows, i:i + 1] * dot_f32(act_refs[i][rows, :], weight_refs[i][...])
            total = term if total is None else total + term
        out_ref[rows, :] = total


def group_down(acts, weights, comb, acc):
    n_act = len(acts)
    rows, ff = acts[0].shape
    d_model = weights[0].shape[2]
    block = 512
    col_map = lambda n: (0, n)
    whole_map = lambda n: (0, 0)
    in_specs = [pl.BlockSpec((rows, ff), whole_map, pipeline_mode=pl.Buffered(1)) for _ in acts]
    in_specs += [pl.BlockSpec((w.shape[0], ff, block), lambda n: (0, 0, n)) for w in weights]
    in_specs.append(pl.BlockSpec((rows, n_act), whole_map))
    operands = [*acts, *weights, comb]
    if acc is not None:
        in_specs.append(pl.BlockSpec((rows, block), col_map))
        operands.append(acc)
    return pl.pallas_call(
        functools.partial(group_down_kernel, n_act, len(weights), acc is not None),
        grid=(d_model // block,),
        in_specs=in_specs,
        out_specs=pl.BlockSpec((rows, block), col_map),
        out_shape=jax.ShapeDtypeStruct((rows, d_model), jnp.float32),
        compiler_params=pltpu.CompilerParams(vmem_limit_bytes=60 * 1024 * 1024),
        cost_estimate=pl.CostEstimate(flops=2 * n_act * rows * ff * d_model, bytes_accessed=rows * d_model * 8, transcendentals=0),
        name='group_down',
    )(*operands)


def last_down_kernel(act_ref, weight_ref, comb_ref, acc_ref, mid_ref, gain_ref, out_ref, sum_ref):
    d_model = out_ref.shape[1]
    step = d_model // 6
    square_sum = jnp.zeros((out_ref.shape[0], 1), jnp.float32)
    for j in range(6):
        cols = slice(j * step, (j + 1) * step)
        part = acc_ref[:, cols] + comb_ref[...] * dot_f32(act_ref[...], weight_ref[:, cols])
        sum_ref[:, cols] = part
        square_sum += jnp.sum(part * part, axis=-1, keepdims=True)
    inv_rms = lax.rsqrt(square_sum * (1.0 / d_model) + NORM_EPS)
    for j in range(6):
        cols = slice(j * step, (j + 1) * step)
        out_ref[:, cols] = (mid_ref[:, cols].astype(jnp.float32) + sum_ref[:, cols] * inv_rms * gain_ref[:, cols]).astype(jnp.bfloat16)


def last_down(act, weight, comb, acc, mid, gain):
    rows, ff = act.shape
    d_model = weight.shape[1]
    block = 256
    row_map = lambda m: (m, 0)
    whole_map = lambda m: (0, 0)
    return pl.pallas_call(
        last_down_kernel,
        grid=(rows // block,),
        in_specs=[
            pl.BlockSpec((block, ff), row_map),
            pl.BlockSpec((ff, d_model), whole_map, pipeline_mode=pl.Buffered(1)),
            pl.BlockSpec((block, 1), row_map),
            pl.BlockSpec((block, d_model), row_map),
            pl.BlockSpec((block, d_model), row_map),
            pl.BlockSpec((1, d_model), whole_map),
        ],
        out_specs=pl.BlockSpec((block, d_model), row_map),
        out_shape=jax.ShapeDtypeStruct((rows, d_model), jnp.bfloat16),
        scratch_shapes=[pltpu.VMEM((block, d_model), jnp.float32)],
        compiler_params=pltpu.CompilerParams(vmem_limit_bytes=60 * 1024 * 1024),
        cost_estimate=pl.CostEstimate(flops=2 * rows * ff * d_model, bytes_accessed=rows * d_model * 8, transcendentals=0),
        name='last_down',
    )(act, weight, comb, acc, mid, gain)


def solution(mesh):
    row_spec = P(('dp', 'wg'))
    dim0_spec = P('wg', None)
    dim1_spec = P(None, 'wg', None)
    gather_dim0 = functools.partial(lax.all_gather, axis_name='wg', axis=0, tiled=True)
    gather_dim1 = functools.partial(lax.all_gather, axis_name='wg', axis=1, tiled=True)

    def device_fn(hidden, seq_lens, route_idx, g_attn_in, w_query, w_key, w_value, w_attn_out, g_attn_out, g_moe_in, w_router, w_gate, w_up, w_down, g_moe_out):
        n_prompts, seq_len, d_model = hidden.shape
        n_experts, local_rows, ff_dim = w_gate.shape
        kv_dim = w_key.shape[1]
        tok_rows = hidden.reshape(n_prompts * seq_len, d_model)
        small = jnp.concatenate([g_attn_in, g_attn_out, g_moe_in, g_moe_out, w_router.T.reshape(-1)])
        small = lax.all_gather(small, 'wg', axis=0, tiled=False)
        n_dev = small.shape[0]
        small = small.reshape(n_dev, 4 + n_experts, -1).transpose(1, 0, 2).reshape(4 + n_experts, d_model)
        h_attn = rms_norm(tok_rows, small[0]).astype(jnp.bfloat16)
        w_query_all = gather_dim0(w_query)
        w_query_all, w_attn_out = lax.optimization_barrier((w_query_all, w_attn_out))
        half_rows = local_rows // 2
        out_top = spread(w_attn_out[:half_rows], True)
        out_low = spread(w_attn_out[half_rows:], False)
        q_proj = dot_f32(h_attn, w_query_all).astype(jnp.bfloat16)
        q_proj, h_attn = lax.optimization_barrier((q_proj, h_attn))
        kv_proj = dot_f32(h_attn, gather_dim0(jnp.concatenate([w_key, w_value], axis=1))).astype(jnp.bfloat16)
        k_proj, v_proj = kv_proj[:, :kv_dim], kv_proj[:, kv_dim:]
        context_rows, k_rope, v_heads = attend_rows(q_proj, k_proj, v_proj, seq_lens)
        context_rows = jnp.concatenate(owner_columns(context_rows, local_rows, 0, half_rows) + owner_columns(context_rows, local_rows, half_rows, half_rows), axis=1)
        w_attn_all = jnp.concatenate(out_top + out_low, axis=0)
        w_attn_all, w_down_perm = lax.optimization_barrier((w_attn_all, w_down[:4]))
        down_01 = spread(w_down_perm[:2], True)
        down_23 = spread(w_down_perm[2:], False)
        attn_out = dot_f32(context_rows, w_attn_all)
        mid_rows = (tok_rows.astype(jnp.float32) + rms_norm(attn_out, small[1])).astype(jnp.bfloat16)
        h_moe = rms_norm(mid_rows, small[2]).astype(jnp.bfloat16)
        logits = lax.dot_general(h_moe, small[4:], (((1,), (1,)), ((), ())), preferred_element_type=jnp.float32)
        router_probs = jax.nn.softmax(logits, axis=-1)
        picks = (route_idx[:, :, None] == jnp.arange(n_experts)).astype(jnp.float32)
        combine = router_probs * jnp.sum(picks, axis=1)

        def inner(h_in, w_gate_e, w_up_e):
            gate_act = dot_f32(h_in, w_gate_e)
            up_act = dot_f32(h_in, w_up_e)
            return (jax.nn.gelu(gate_act) * up_act).astype(jnp.bfloat16)

        ff_rows = ff_dim // n_dev
        acts = []
        for lo, hi in ((0, 4), (4, 8)):
            n_part = hi - lo
            packed = gather_dim1(jnp.concatenate([w_gate[lo:hi], w_up[lo:hi]], axis=0))
            for i in range(n_part):
                act = inner(h_moe, packed[i], packed[n_part + i])
                if lo + i == 3:
                    down_01 = jnp.concatenate(down_01, axis=1)
                    down_23 = jnp.concatenate(down_23, axis=1)
                    act, h_moe, down_01, down_23 = lax.optimization_barrier((act, h_moe, down_01, down_23))
                else:
                    act, h_moe = lax.optimization_barrier((act, h_moe))
                acts.append(act)
            if lo == 0:
                owned = [jnp.concatenate(owner_columns(act, ff_rows, 0, ff_rows), axis=1) for act in acts]
                moe_acc = group_down(owned, [down_01, down_23], combine[:, :4], None)
                moe_acc, h_moe = lax.optimization_barrier((moe_acc, h_moe))
        moe_acc = group_down(acts[4:7], [gather_dim1(w_down[4:7])], combine[:, 4:7], moe_acc)
        act_7, down_7 = acts[7], gather_dim1(w_down[7:8])[0]
        y_rows = last_down(act_7, down_7, combine[:, 7:8], moe_acc, mid_rows, small[3].astype(jnp.float32)[None])
        return y_rows.reshape(hidden.shape), k_rope, v_heads

    return jax.shard_map(
        device_fn,
        mesh=mesh,
        in_specs=(row_spec, row_spec, row_spec, P('wg'), dim0_spec, dim0_spec, dim0_spec, dim0_spec, P('wg'), P('wg'), dim0_spec, dim1_spec, dim1_spec, dim1_spec, P('wg')),
        out_specs=(row_spec, row_spec, row_spec),
        check_vma=False,
    )
```

```python
import functools
import jax
import jax.numpy as jnp
from jax import lax
from jax.experimental import pallas as pl
from jax.experimental.pallas import tpu as pltpu
from jax.sharding import PartitionSpec as P

HEAD_DIM = 128
SOFT_CAP = 30.0
NORM_EPS = 1e-5
ROPE_BASE = 10000.0
ATTN_SCALE = HEAD_DIM ** -0.5


def dot_f32(left_op, right_op):
    return jnp.dot(left_op, right_op, preferred_element_type=jnp.float32)


def rms_norm(values, gain_vec):
    values_f32 = values.astype(jnp.float32)
    inv_rms = lax.rsqrt(jnp.mean(values_f32 * values_f32, axis=-1, keepdims=True) + NORM_EPS)
    return values_f32 * inv_rms * gain_vec.astype(jnp.float32)


def rope_tables(seq_len):
    half_dim = HEAD_DIM // 2
    inv_freq = ROPE_BASE ** (-jnp.arange(half_dim, dtype=jnp.float32) * (2.0 / HEAD_DIM))
    angles = jnp.arange(seq_len, dtype=jnp.float32)[:, None] * inv_freq[None, :]
    return jnp.cos(angles)[:, None, :], jnp.sin(angles)[:, None, :]


def apply_rope(values, cos_t, sin_t):
    half_dim = HEAD_DIM // 2
    values_f32 = values.astype(jnp.float32)
    first_half = values_f32[..., :half_dim]
    second_half = values_f32[..., half_dim:]
    return jnp.concatenate([first_half * cos_t - second_half * sin_t, second_half * cos_t + first_half * sin_t], axis=-1).astype(jnp.bfloat16)


def attend_prompt(operands):
    q_rows, k_rows, v_rows, length = operands
    positions = jnp.arange(q_rows.shape[0])
    scores = jnp.einsum('qkgd,skd->kgqs', q_rows, k_rows, preferred_element_type=jnp.float32) * ATTN_SCALE
    scores = SOFT_CAP * jnp.tanh(scores / SOFT_CAP)
    allowed = (positions[None, :] <= positions[:, None]) & (positions[None, :] < length)
    scores = jnp.where(allowed, scores, -1e30)
    attn_probs = jax.nn.softmax(scores, axis=-1).astype(jnp.bfloat16)
    return jnp.einsum('kgqs,skd->qkgd', attn_probs, v_rows, preferred_element_type=jnp.float32).astype(jnp.bfloat16)


def attend_rows(q_proj, k_proj, v_proj, seq_lens):
    n_prompts = seq_lens.shape[0]
    seq_len = q_proj.shape[0] // n_prompts
    n_heads = q_proj.shape[1] // HEAD_DIM
    n_kv = k_proj.shape[1] // HEAD_DIM
    cos_t, sin_t = rope_tables(seq_len)
    q_rope = apply_rope(q_proj.reshape(n_prompts, seq_len, n_heads, HEAD_DIM), cos_t, sin_t)
    k_rope = apply_rope(k_proj.reshape(n_prompts, seq_len, n_kv, HEAD_DIM), cos_t, sin_t)
    v_heads = v_proj.reshape(n_prompts, seq_len, n_kv, HEAD_DIM)
    q_groups = q_rope.reshape(n_prompts, seq_len, n_kv, n_heads // n_kv, HEAD_DIM)
    context = lax.map(attend_prompt, (q_groups, k_rope, v_heads, seq_lens))
    return context.reshape(n_prompts * seq_len, n_heads * HEAD_DIM), k_rope, v_heads


PIECE_ORDER = (0, 2, 4, 6, 1, 3, 5, 7)


def swap(values, distance):
    return lax.ppermute(values, 'wg', [(d, d ^ distance) for d in range(8)])


def to_neighbours(piece):
    return swap(piece, 2), swap(piece, 4)


def all_pieces(piece, from_x, from_y, over_y):
    from_diag = swap(from_x, 4) if over_y else swap(from_y, 2)
    own = [piece, from_x, from_y, from_diag]
    return own + [swap(part, 1) for part in own]


def owner_columns(values, chunk, start, width):
    me = lax.axis_index('wg')
    return [lax.dynamic_slice_in_dim(values, (me ^ o) * chunk + start, width, axis=1) for o in PIECE_ORDER]


def group_down_kernel(n_act, n_weight, has_acc, *refs):
    act_refs = refs[:n_act]
    weight_refs = [ref.at[i] for ref in refs[n_act:n_act + n_weight] for i in range(ref.shape[0])]
    comb_ref = refs[n_act + n_weight]
    acc_ref = refs[n_act + n_weight + 1] if has_acc else None
    out_ref = refs[-1]
    block = 512

    @pl.loop(0, out_ref.shape[0] // block)
    def _(m):
        rows = pl.ds(pl.multiple_of(m * block, block), block)
        total = acc_ref[rows, :] if has_acc else None
        for i in range(n_act):
            term = comb_ref[rows, i:i + 1] * dot_f32(act_refs[i][rows, :], weight_refs[i][...])
            total = term if total is None else total + term
        out_ref[rows, :] = total


def group_down(acts, weights, comb, acc):
    n_act = len(acts)
    rows, ff = acts[0].shape
    d_model = weights[0].shape[2]
    block = 512
    col_map = lambda n: (0, n)
    whole_map = lambda n: (0, 0)
    in_specs = [pl.BlockSpec((rows, ff), whole_map, pipeline_mode=pl.Buffered(1)) for _ in acts]
    in_specs += [pl.BlockSpec((w.shape[0], ff, block), lambda n: (0, 0, n)) for w in weights]
    in_specs.append(pl.BlockSpec((rows, n_act), whole_map))
    operands = [*acts, *weights, comb]
    if acc is not None:
        in_specs.append(pl.BlockSpec((rows, block), col_map))
        operands.append(acc)
    return pl.pallas_call(
        functools.partial(group_down_kernel, n_act, len(weights), acc is not None),
        grid=(d_model // block,),
        in_specs=in_specs,
        out_specs=pl.BlockSpec((rows, block), col_map),
        out_shape=jax.ShapeDtypeStruct((rows, d_model), jnp.float32),
        compiler_params=pltpu.CompilerParams(vmem_limit_bytes=60 * 1024 * 1024),
        cost_estimate=pl.CostEstimate(flops=2 * n_act * rows * ff * d_model, bytes_accessed=rows * d_model * 8, transcendentals=0),
        name='group_down',
    )(*operands)


def last_down_kernel(act_ref, weight_ref, comb_ref, acc_ref, mid_ref, gain_ref, out_ref, sum_ref):
    d_model = out_ref.shape[1]
    step = d_model // 6
    square_sum = jnp.zeros((out_ref.shape[0], 1), jnp.float32)
    for j in range(6):
        cols = slice(j * step, (j + 1) * step)
        part = acc_ref[:, cols] + comb_ref[...] * dot_f32(act_ref[...], weight_ref[:, cols])
        sum_ref[:, cols] = part
        square_sum += jnp.sum(part * part, axis=-1, keepdims=True)
    inv_rms = lax.rsqrt(square_sum * (1.0 / d_model) + NORM_EPS)
    for j in range(6):
        cols = slice(j * step, (j + 1) * step)
        out_ref[:, cols] = (mid_ref[:, cols].astype(jnp.float32) + sum_ref[:, cols] * inv_rms * gain_ref[:, cols]).astype(jnp.bfloat16)


def last_down(act, weight, comb, acc, mid, gain):
    rows, ff = act.shape
    d_model = weight.shape[1]
    block = 256
    row_map = lambda m: (m, 0)
    whole_map = lambda m: (0, 0)
    return pl.pallas_call(
        last_down_kernel,
        grid=(rows // block,),
        in_specs=[
            pl.BlockSpec((block, ff), row_map),
            pl.BlockSpec((ff, d_model), whole_map, pipeline_mode=pl.Buffered(1)),
            pl.BlockSpec((block, 1), row_map),
            pl.BlockSpec((block, d_model), row_map),
            pl.BlockSpec((block, d_model), row_map),
            pl.BlockSpec((1, d_model), whole_map),
        ],
        out_specs=pl.BlockSpec((block, d_model), row_map),
        out_shape=jax.ShapeDtypeStruct((rows, d_model), jnp.bfloat16),
        scratch_shapes=[pltpu.VMEM((block, d_model), jnp.float32)],
        compiler_params=pltpu.CompilerParams(vmem_limit_bytes=60 * 1024 * 1024),
        cost_estimate=pl.CostEstimate(flops=2 * rows * ff * d_model, bytes_accessed=rows * d_model * 8, transcendentals=0),
        name='last_down',
    )(act, weight, comb, acc, mid, gain)


def solution(mesh):
    row_spec = P(('dp', 'wg'))
    dim0_spec = P('wg', None)
    dim1_spec = P(None, 'wg', None)
    gather_dim0 = functools.partial(lax.all_gather, axis_name='wg', axis=0, tiled=True)
    gather_dim1 = functools.partial(lax.all_gather, axis_name='wg', axis=1, tiled=True)

    def device_fn(hidden, seq_lens, route_idx, g_attn_in, w_query, w_key, w_value, w_attn_out, g_attn_out, g_moe_in, w_router, w_gate, w_up, w_down, g_moe_out):
        n_prompts, seq_len, d_model = hidden.shape
        n_experts, local_rows, ff_dim = w_gate.shape
        kv_dim = w_key.shape[1]
        tok_rows = hidden.reshape(n_prompts * seq_len, d_model)
        small = jnp.concatenate([g_attn_in, g_attn_out, g_moe_in, g_moe_out, w_router.T.reshape(-1)])
        small = lax.all_gather(small, 'wg', axis=0, tiled=False)
        n_dev = small.shape[0]
        small = small.reshape(n_dev, 4 + n_experts, -1).transpose(1, 0, 2).reshape(4 + n_experts, d_model)
        h_attn = rms_norm(tok_rows, small[0]).astype(jnp.bfloat16)
        w_query_all = gather_dim0(w_query)
        w_query_all, w_attn_out = lax.optimization_barrier((w_query_all, w_attn_out))
        half_rows = local_rows // 2
        top_piece, low_piece = w_attn_out[:half_rows], w_attn_out[half_rows:]
        top_x, top_y = to_neighbours(top_piece)
        low_x, low_y = to_neighbours(low_piece)
        q_proj = dot_f32(h_attn, w_query_all).astype(jnp.bfloat16)
        q_proj, h_attn, top_x, low_y = lax.optimization_barrier((q_proj, h_attn, top_x, low_y))
        out_top = all_pieces(top_piece, top_x, top_y, True)
        out_low = all_pieces(low_piece, low_x, low_y, False)
        kv_proj = dot_f32(h_attn, gather_dim0(jnp.concatenate([w_key, w_value], axis=1))).astype(jnp.bfloat16)
        k_proj, v_proj = kv_proj[:, :kv_dim], kv_proj[:, kv_dim:]
        context_rows, k_rope, v_heads = attend_rows(q_proj, k_proj, v_proj, seq_lens)
        context_rows = jnp.concatenate(owner_columns(context_rows, local_rows, 0, half_rows) + owner_columns(context_rows, local_rows, half_rows, half_rows), axis=1)
        w_attn_all = jnp.concatenate(out_top + out_low, axis=0)
        w_attn_all, gate_perm, up_perm = lax.optimization_barrier((w_attn_all, w_gate[:2], w_up[:2]))
        piece_0 = jnp.concatenate([gate_perm[:1], up_perm[:1]], axis=0)
        piece_1 = jnp.concatenate([gate_perm[1:], up_perm[1:]], axis=0)
        piece_0_x, piece_0_y = to_neighbours(piece_0)
        piece_1_x, piece_1_y = to_neighbours(piece_1)
        attn_out = dot_f32(context_rows, w_attn_all)
        mid_rows = (tok_rows.astype(jnp.float32) + rms_norm(attn_out, small[1])).astype(jnp.bfloat16)
        h_moe = rms_norm(mid_rows, small[2]).astype(jnp.bfloat16)
        logits = lax.dot_general(h_moe, small[4:], (((1,), (1,)), ((), ())), preferred_element_type=jnp.float32)
        router_probs = jax.nn.softmax(logits, axis=-1)
        picks = (route_idx[:, :, None] == jnp.arange(n_experts)).astype(jnp.float32)
        combine = router_probs * jnp.sum(picks, axis=1)

        def inner(h_in, w_gate_e, w_up_e):
            gate_act = dot_f32(h_in, w_gate_e)
            up_act = dot_f32(h_in, w_up_e)
            return (jax.nn.gelu(gate_act) * up_act).astype(jnp.bfloat16)

        acts = [None] * n_experts

        def gathered_experts(lo, hi, h_in):
            n_part = hi - lo
            packed = gather_dim1(jnp.concatenate([w_gate[lo:hi], w_up[lo:hi]], axis=0))
            for i in range(n_part):
                act = inner(h_in, packed[i], packed[n_part + i])
                acts[lo + i], h_in = lax.optimization_barrier((act, h_in))
            return h_in

        h_moe = gathered_experts(2, 4, h_moe)
        h_moe, piece_0_x, piece_1_y = lax.optimization_barrier((h_moe, piece_0_x, piece_1_y))
        h_owned = jnp.concatenate(owner_columns(h_moe, local_rows, 0, local_rows), axis=1)
        for e, pieces in enumerate((all_pieces(piece_0, piece_0_x, piece_0_y, True), all_pieces(piece_1, piece_1_x, piece_1_y, False))):
            w_both = jnp.concatenate(pieces, axis=1)
            act = inner(h_owned, w_both[0], w_both[1])
            acts[e], h_owned, h_moe = lax.optimization_barrier((act, h_owned, h_moe))
        gathered_experts(4, 8, h_moe)
        acts = list(lax.optimization_barrier(tuple(acts)))
        moe_acc = None
        for lo, hi in ((0, 4), (4, 7)):
            moe_acc = group_down(acts[lo:hi], [gather_dim1(w_down[lo:hi])], combine[:, lo:hi], moe_acc)
        act_7, down_7 = acts[7], gather_dim1(w_down[7:8])[0]
        y_rows = last_down(act_7, down_7, combine[:, 7:8], moe_acc, mid_rows, small[3].astype(jnp.float32)[None])
        return y_rows.reshape(hidden.shape), k_rope, v_heads

    return jax.shard_map(
        device_fn,
        mesh=mesh,
        in_specs=(row_spec, row_spec, row_spec, P('wg'), dim0_spec, dim0_spec, dim0_spec, dim0_spec, P('wg'), P('wg'), dim0_spec, dim1_spec, dim1_spec, dim1_spec, P('wg')),
        out_specs=(row_spec, row_spec, row_spec),
        check_vma=False,
    )
```

```python
import functools
import jax
import jax.numpy as jnp
from jax import lax
from jax.experimental import pallas as pl
from jax.experimental.pallas import tpu as pltpu
from jax.sharding import PartitionSpec as P

HEAD_DIM = 128
SOFT_CAP = 30.0
NORM_EPS = 1e-5
ROPE_BASE = 10000.0
ATTN_SCALE = HEAD_DIM ** -0.5


def dot_f32(left_op, right_op):
    return jnp.dot(left_op, right_op, preferred_element_type=jnp.float32)


def rms_norm(values, gain_vec):
    values_f32 = values.astype(jnp.float32)
    inv_rms = lax.rsqrt(jnp.mean(values_f32 * values_f32, axis=-1, keepdims=True) + NORM_EPS)
    return values_f32 * inv_rms * gain_vec.astype(jnp.float32)


def rope_tables(seq_len):
    half_dim = HEAD_DIM // 2
    inv_freq = ROPE_BASE ** (-jnp.arange(half_dim, dtype=jnp.float32) * (2.0 / HEAD_DIM))
    angles = jnp.arange(seq_len, dtype=jnp.float32)[:, None] * inv_freq[None, :]
    return jnp.cos(angles)[:, None, :], jnp.sin(angles)[:, None, :]


def apply_rope(values, cos_t, sin_t):
    half_dim = HEAD_DIM // 2
    values_f32 = values.astype(jnp.float32)
    first_half = values_f32[..., :half_dim]
    second_half = values_f32[..., half_dim:]
    return jnp.concatenate([first_half * cos_t - second_half * sin_t, second_half * cos_t + first_half * sin_t], axis=-1).astype(jnp.bfloat16)


def attend_prompt(operands):
    q_rows, k_rows, v_rows, length = operands
    positions = jnp.arange(q_rows.shape[0])
    scores = jnp.einsum('qkgd,skd->kgqs', q_rows, k_rows, preferred_element_type=jnp.float32) * ATTN_SCALE
    scores = SOFT_CAP * jnp.tanh(scores / SOFT_CAP)
    allowed = (positions[None, :] <= positions[:, None]) & (positions[None, :] < length)
    scores = jnp.where(allowed, scores, -1e30)
    attn_probs = jax.nn.softmax(scores, axis=-1).astype(jnp.bfloat16)
    return jnp.einsum('kgqs,skd->qkgd', attn_probs, v_rows, preferred_element_type=jnp.float32).astype(jnp.bfloat16)


def attend_rows(q_proj, k_proj, v_proj, seq_lens):
    n_prompts = seq_lens.shape[0]
    seq_len = q_proj.shape[0] // n_prompts
    n_heads = q_proj.shape[1] // HEAD_DIM
    n_kv = k_proj.shape[1] // HEAD_DIM
    cos_t, sin_t = rope_tables(seq_len)
    q_rope = apply_rope(q_proj.reshape(n_prompts, seq_len, n_heads, HEAD_DIM), cos_t, sin_t)
    k_rope = apply_rope(k_proj.reshape(n_prompts, seq_len, n_kv, HEAD_DIM), cos_t, sin_t)
    v_heads = v_proj.reshape(n_prompts, seq_len, n_kv, HEAD_DIM)
    q_groups = q_rope.reshape(n_prompts, seq_len, n_kv, n_heads // n_kv, HEAD_DIM)
    context = lax.map(attend_prompt, (q_groups, k_rope, v_heads, seq_lens))
    return context.reshape(n_prompts * seq_len, n_heads * HEAD_DIM), k_rope, v_heads


PIECE_ORDER = (0, 2, 4, 6, 1, 3, 5, 7)


def swap(values, distance):
    return lax.ppermute(values, 'wg', [(d, d ^ distance) for d in range(8)])


def to_neighbours(piece):
    return swap(piece, 2), swap(piece, 4)


def all_pieces(piece, from_x, from_y, over_y):
    from_diag = swap(from_x, 4) if over_y else swap(from_y, 2)
    own = [piece, from_x, from_y, from_diag]
    return own + [swap(part, 1) for part in own]


def owner_columns(values, chunk, start, width):
    me = lax.axis_index('wg')
    return [lax.dynamic_slice_in_dim(values, (me ^ o) * chunk + start, width, axis=1) for o in PIECE_ORDER]


def group_down_kernel(n_act, n_weight, has_acc, *refs):
    act_refs = refs[:n_act]
    weight_refs = [ref.at[i] for ref in refs[n_act:n_act + n_weight] for i in range(ref.shape[0])]
    comb_ref = refs[n_act + n_weight]
    acc_ref = refs[n_act + n_weight + 1] if has_acc else None
    out_ref = refs[-1]
    block = 512

    @pl.loop(0, out_ref.shape[0] // block)
    def _(m):
        rows = pl.ds(pl.multiple_of(m * block, block), block)
        total = acc_ref[rows, :] if has_acc else None
        for i in range(n_act):
            term = comb_ref[rows, i:i + 1] * dot_f32(act_refs[i][rows, :], weight_refs[i][...])
            total = term if total is None else total + term
        out_ref[rows, :] = total


def group_down(acts, weights, comb, acc):
    n_act = len(acts)
    rows, ff = acts[0].shape
    d_model = weights[0].shape[2]
    block = 512
    col_map = lambda n: (0, n)
    whole_map = lambda n: (0, 0)
    in_specs = [pl.BlockSpec((rows, ff), whole_map, pipeline_mode=pl.Buffered(1)) for _ in acts]
    in_specs += [pl.BlockSpec((w.shape[0], ff, block), lambda n: (0, 0, n)) for w in weights]
    in_specs.append(pl.BlockSpec((rows, n_act), whole_map))
    operands = [*acts, *weights, comb]
    if acc is not None:
        in_specs.append(pl.BlockSpec((rows, block), col_map))
        operands.append(acc)
    return pl.pallas_call(
        functools.partial(group_down_kernel, n_act, len(weights), acc is not None),
        grid=(d_model // block,),
        in_specs=in_specs,
        out_specs=pl.BlockSpec((rows, block), col_map),
        out_shape=jax.ShapeDtypeStruct((rows, d_model), jnp.float32),
        compiler_params=pltpu.CompilerParams(vmem_limit_bytes=60 * 1024 * 1024),
        cost_estimate=pl.CostEstimate(flops=2 * n_act * rows * ff * d_model, bytes_accessed=rows * d_model * 8, transcendentals=0),
        name='group_down',
    )(*operands)


def last_down_kernel(act_ref, weight_ref, comb_ref, acc_ref, mid_ref, gain_ref, out_ref, sum_ref):
    d_model = out_ref.shape[1]
    step = d_model // 6
    square_sum = jnp.zeros((out_ref.shape[0], 1), jnp.float32)
    for j in range(6):
        cols = slice(j * step, (j + 1) * step)
        part = acc_ref[:, cols] + comb_ref[...] * dot_f32(act_ref[...], weight_ref[:, cols])
        sum_ref[:, cols] = part
        square_sum += jnp.sum(part * part, axis=-1, keepdims=True)
    inv_rms = lax.rsqrt(square_sum * (1.0 / d_model) + NORM_EPS)
    for j in range(6):
        cols = slice(j * step, (j + 1) * step)
        out_ref[:, cols] = (mid_ref[:, cols].astype(jnp.float32) + sum_ref[:, cols] * inv_rms * gain_ref[:, cols]).astype(jnp.bfloat16)


def last_down(act, weight, comb, acc, mid, gain):
    rows, ff = act.shape
    d_model = weight.shape[1]
    block = 256
    row_map = lambda m: (m, 0)
    whole_map = lambda m: (0, 0)
    return pl.pallas_call(
        last_down_kernel,
        grid=(rows // block,),
        in_specs=[
            pl.BlockSpec((block, ff), row_map),
            pl.BlockSpec((ff, d_model), whole_map, pipeline_mode=pl.Buffered(1)),
            pl.BlockSpec((block, 1), row_map),
            pl.BlockSpec((block, d_model), row_map),
            pl.BlockSpec((block, d_model), row_map),
            pl.BlockSpec((1, d_model), whole_map),
        ],
        out_specs=pl.BlockSpec((block, d_model), row_map),
        out_shape=jax.ShapeDtypeStruct((rows, d_model), jnp.bfloat16),
        scratch_shapes=[pltpu.VMEM((block, d_model), jnp.float32)],
        compiler_params=pltpu.CompilerParams(vmem_limit_bytes=60 * 1024 * 1024),
        cost_estimate=pl.CostEstimate(flops=2 * rows * ff * d_model, bytes_accessed=rows * d_model * 8, transcendentals=0),
        name='last_down',
    )(act, weight, comb, acc, mid, gain)


def solution(mesh):
    row_spec = P(('dp', 'wg'))
    dim0_spec = P('wg', None)
    dim1_spec = P(None, 'wg', None)
    gather_dim0 = functools.partial(lax.all_gather, axis_name='wg', axis=0, tiled=True)
    gather_dim1 = functools.partial(lax.all_gather, axis_name='wg', axis=1, tiled=True)

    def device_fn(hidden, seq_lens, route_idx, g_attn_in, w_query, w_key, w_value, w_attn_out, g_attn_out, g_moe_in, w_router, w_gate, w_up, w_down, g_moe_out):
        n_prompts, seq_len, d_model = hidden.shape
        n_experts, local_rows, ff_dim = w_gate.shape
        kv_dim = w_key.shape[1]
        tok_rows = hidden.reshape(n_prompts * seq_len, d_model)
        small = jnp.concatenate([g_attn_in, g_attn_out, g_moe_in, g_moe_out, w_router.T.reshape(-1)])
        small = lax.all_gather(small, 'wg', axis=0, tiled=False)
        n_dev = small.shape[0]
        small = small.reshape(n_dev, 4 + n_experts, -1).transpose(1, 0, 2).reshape(4 + n_experts, d_model)
        h_attn = rms_norm(tok_rows, small[0]).astype(jnp.bfloat16)
        w_query_all = gather_dim0(w_query)
        w_query_all, w_attn_out = lax.optimization_barrier((w_query_all, w_attn_out))
        half_rows = local_rows // 2
        top_piece, low_piece = w_attn_out[:half_rows], w_attn_out[half_rows:]
        top_x, low_y = swap(top_piece, 2), swap(low_piece, 4)
        q_proj = dot_f32(h_attn, w_query_all).astype(jnp.bfloat16)
        q_proj, h_attn, top_x, low_y, top_piece, low_piece = lax.optimization_barrier((q_proj, h_attn, top_x, low_y, top_piece, low_piece))
        top_y, low_x = swap(top_piece, 4), swap(low_piece, 2)
        out_top = all_pieces(top_piece, top_x, top_y, True)
        out_low = all_pieces(low_piece, low_x, low_y, False)
        kv_proj = dot_f32(h_attn, gather_dim0(jnp.concatenate([w_key, w_value], axis=1))).astype(jnp.bfloat16)
        k_proj, v_proj = kv_proj[:, :kv_dim], kv_proj[:, kv_dim:]
        context_rows, k_rope, v_heads = attend_rows(q_proj, k_proj, v_proj, seq_lens)
        context_rows = jnp.concatenate(owner_columns(context_rows, local_rows, 0, half_rows) + owner_columns(context_rows, local_rows, half_rows, half_rows), axis=1)
        w_attn_all = jnp.concatenate(out_top + out_low, axis=0)
        w_attn_all, gate_perm, up_perm = lax.optimization_barrier((w_attn_all, w_gate[:2], w_up[:2]))
        piece_0 = jnp.concatenate([gate_perm[:1], up_perm[:1]], axis=0)
        piece_1 = jnp.concatenate([gate_perm[1:], up_perm[1:]], axis=0)
        piece_0_x, piece_0_y = to_neighbours(piece_0)
        piece_1_x, piece_1_y = to_neighbours(piece_1)
        attn_out = dot_f32(context_rows, w_attn_all)
        mid_rows = (tok_rows.astype(jnp.float32) + rms_norm(attn_out, small[1])).astype(jnp.bfloat16)
        h_moe = rms_norm(mid_rows, small[2]).astype(jnp.bfloat16)
        logits = lax.dot_general(h_moe, small[4:], (((1,), (1,)), ((), ())), preferred_element_type=jnp.float32)
        router_probs = jax.nn.softmax(logits, axis=-1)
        picks = (route_idx[:, :, None] == jnp.arange(n_experts)).astype(jnp.float32)
        combine = router_probs * jnp.sum(picks, axis=1)

        def inner(h_in, w_gate_e, w_up_e):
            gate_act = dot_f32(h_in, w_gate_e)
            up_act = dot_f32(h_in, w_up_e)
            return (jax.nn.gelu(gate_act) * up_act).astype(jnp.bfloat16)

        acts = [None] * n_experts

        def gathered_experts(lo, hi, h_in):
            n_part = hi - lo
            packed = gather_dim1(jnp.concatenate([w_gate[lo:hi], w_up[lo:hi]], axis=0))
            for i in range(n_part):
                act = inner(h_in, packed[i], packed[n_part + i])
                acts[lo + i], h_in = lax.optimization_barrier((act, h_in))
            return h_in

        h_moe = gathered_experts(2, 4, h_moe)
        h_moe, piece_0_x, piece_1_y = lax.optimization_barrier((h_moe, piece_0_x, piece_1_y))
        h_owned = jnp.concatenate(owner_columns(h_moe, local_rows, 0, local_rows), axis=1)
        for e, pieces in enumerate((all_pieces(piece_0, piece_0_x, piece_0_y, True), all_pieces(piece_1, piece_1_x, piece_1_y, False))):
            w_both = jnp.concatenate(pieces, axis=1)
            act = inner(h_owned, w_both[0], w_both[1])
            acts[e], h_owned, h_moe = lax.optimization_barrier((act, h_owned, h_moe))
        gathered_experts(4, 8, h_moe)
        acts = list(lax.optimization_barrier(tuple(acts)))
        moe_acc = None
        for lo, hi in ((0, 4), (4, 7)):
            moe_acc = group_down(acts[lo:hi], [gather_dim1(w_down[lo:hi])], combine[:, lo:hi], moe_acc)
        act_7, down_7 = acts[7], gather_dim1(w_down[7:8])[0]
        y_rows = last_down(act_7, down_7, combine[:, 7:8], moe_acc, mid_rows, small[3].astype(jnp.float32)[None])
        return y_rows.reshape(hidden.shape), k_rope, v_heads

    return jax.shard_map(
        device_fn,
        mesh=mesh,
        in_specs=(row_spec, row_spec, row_spec, P('wg'), dim0_spec, dim0_spec, dim0_spec, dim0_spec, P('wg'), P('wg'), dim0_spec, dim1_spec, dim1_spec, dim1_spec, P('wg')),
        out_specs=(row_spec, row_spec, row_spec),
        check_vma=False,
    )
```
